128 devices in a mesh: sub: 4 (over x), fsdp: 32 (over z, y, core).
Axes of the slice: x: 4, y: 4, z: 4, core: 2. Of those that a mesh axis runs over, the one named last changes fastest.
Arguments:
- x_in: bfloat16 [128, 192, 1536], P(('sub', 'fsdp'))
- w_q: bfloat16 [2, 1536, 12, 128], P(None, ('sub', 'fsdp'))
- w_k: bfloat16 [2, 1536, 2, 128], P(None, ('sub', 'fsdp'))
- w_v: bfloat16 [2, 1536, 2, 128], P(None, ('sub', 'fsdp'))
- w_o: bfloat16 [2, 1536, 12, 128], P(None, ('sub', 'fsdp'))
- w_up: bfloat16 [2, 1536, 8960], P(None, ('sub', 'fsdp'))
- w_down: bfloat16 [2, 8960, 1536], P(None, ('sub', 'fsdp'))
- grad_out: bfloat16 [128, 192, 1536], P(('sub', 'fsdp'))
Outputs:
- output 1: bfloat16 [128, 192, 1536], P(('sub', 'fsdp'))
- output 2: bfloat16 [128, 192, 1536], P(('sub', 'fsdp'))
- output 3: float32 [2, 1536, 12, 128], P(None, ('sub', 'fsdp'))
- output 4: float32 [2, 1536, 2, 128], P(None, ('sub', 'fsdp'))
- output 5: float32 [2, 1536, 2, 128], P(None, ('sub', 'fsdp'))
- output 6: float32 [2, 1536, 12, 128], P(None, ('sub', 'fsdp'))
- output 7: float32 [2, 1536, 8960], P(None, ('sub', 'fsdp'))
- output 8: float32 [2, 8960, 1536], P(None, ('sub', 'fsdp'))
All inputs are finite; a program needn't handle non-finite values.
Results may differ from the reference program's by a relative error of at most 0.02.
Values are sent between devices in bfloat16 or wider.
A program may use at most 1 GiB of HBM per device.

```python
import jax
import jax.numpy as jnp
from jax import lax

D = 1536
FF = 8960
HEADS = 12
KV_HEADS = 2
HEAD = 128
SEQ = 192
SEQS_DEV = 1
BLOCKS = 128
PAIRS = 2
EPS = 1e-6
MASK_FILL = -1e30

SEQS = BLOCKS * SEQS_DEV
ROWS = SEQS_DEV * SEQ
Q_PER_KV = HEADS // KV_HEADS
Q_WIDTH = HEADS * HEAD
KV_WIDTH = KV_HEADS * HEAD
SCALE = HEAD ** -0.5


def setup_inputs(seed: int = 0) -> dict:
    key_list = jax.random.split(jax.random.key(seed), 8)
    x_in = jax.random.normal(key_list[0], (SEQS, SEQ, D), jnp.float32)
    w_q = jax.random.normal(key_list[1], (PAIRS, D, HEADS, HEAD), jnp.float32) * D ** -0.5
    w_k = jax.random.normal(key_list[2], (PAIRS, D, KV_HEADS, HEAD), jnp.float32) * D ** -0.5
    w_v = jax.random.normal(key_list[3], (PAIRS, D, KV_HEADS, HEAD), jnp.float32) * D ** -0.5
    w_o = jax.random.normal(key_list[4], (PAIRS, D, HEADS, HEAD), jnp.float32) * (2.0 * (Q_WIDTH * PAIRS) ** -0.5)
    w_up = jax.random.normal(key_list[5], (PAIRS, D, FF), jnp.float32) * D ** -0.5
    w_down = jax.random.normal(key_list[6], (PAIRS, FF, D), jnp.float32) * (1.5 * (FF * PAIRS) ** -0.5)
    grad_out = jax.random.normal(key_list[7], (SEQS, SEQ, D), jnp.float32)
    arrays = {"x_in": x_in, "w_q": w_q, "w_k": w_k, "w_v": w_v, "w_o": w_o, "w_up": w_up, "w_down": w_down, "grad_out": grad_out}
    return {name: value.astype(jnp.bfloat16) for name, value in arrays.items()}


def rms_norm(values):
    return values * lax.rsqrt(jnp.mean(values * values, axis=-1, keepdims=True) + EPS)


def norm_bf16(x_blk):
    return rms_norm(x_blk.astype(jnp.float32)).astype(jnp.bfloat16)


def norm_back(x_blk, grad_norm):
    _, pull_back = jax.vjp(rms_norm, x_blk.astype(jnp.float32))
    return pull_back(grad_norm)[0]


def matmul(left, right):
    return jnp.dot(left, right, preferred_element_type=jnp.float32)


def attn_inner(x_blk, q_weight, k_weight, v_weight):
    normed = norm_bf16(x_blk)
    q_act = matmul(normed, q_weight.reshape(D, Q_WIDTH)).astype(jnp.bfloat16)
    k_act = matmul(normed, k_weight.reshape(D, KV_WIDTH)).astype(jnp.bfloat16)
    v_act = matmul(normed, v_weight.reshape(D, KV_WIDTH)).astype(jnp.bfloat16)
    q_grid = q_act.reshape(SEQS_DEV, SEQ, KV_HEADS, Q_PER_KV, HEAD).astype(jnp.float32)
    k_grid = k_act.reshape(SEQS_DEV, SEQ, KV_HEADS, HEAD).astype(jnp.float32)
    v_grid = v_act.reshape(SEQS_DEV, SEQ, KV_HEADS, HEAD).astype(jnp.float32)
    scores = jnp.einsum("bskge,btke->bkgst", q_grid, k_grid) * SCALE
    positions = jnp.arange(SEQ)
    causal = positions[:, None] >= positions[None, :]
    p_float = jax.nn.softmax(jnp.where(causal, scores, MASK_FILL), axis=-1)
    p_bf16 = p_float.astype(jnp.bfloat16)
    o_act = jnp.einsum("bkgst,btke->bskge", p_bf16.astype(jnp.float32), v_grid).astype(jnp.bfloat16)
    return normed, q_grid, k_grid, v_grid, p_float, p_bf16, o_act.reshape(ROWS, Q_WIDTH)


def attn_forward(x_blk, q_weight, k_weight, v_weight, o_weight):
    o_act = attn_inner(x_blk, q_weight, k_weight, v_weight)[6]
    proj = matmul(o_act, o_weight.reshape(D, Q_WIDTH).T)
    return (x_blk.astype(jnp.float32) + proj).astype(jnp.bfloat16)


def attn_backward(x_blk, q_weight, k_weight, v_weight, o_weight, grad_y):
    normed, q_grid, k_grid, v_grid, p_float, p_bf16, o_act = attn_inner(x_blk, q_weight, k_weight, v_weight)
    q_mat = q_weight.reshape(D, Q_WIDTH)
    k_mat = k_weight.reshape(D, KV_WIDTH)
    v_mat = v_weight.reshape(D, KV_WIDTH)
    d_o_w = matmul(grad_y.T, o_act)
    d_o = matmul(grad_y, o_weight.reshape(D, Q_WIDTH)).astype(jnp.bfloat16)
    d_o_grid = d_o.reshape(SEQS_DEV, SEQ, KV_HEADS, Q_PER_KV, HEAD).astype(jnp.float32)
    d_p = jnp.einsum("bskge,btke->bkgst", d_o_grid, v_grid)
    d_v = jnp.einsum("bkgst,bskge->btke", p_bf16.astype(jnp.float32), d_o_grid).astype(jnp.bfloat16)
    d_s = p_float * (d_p - jnp.sum(p_float * d_p, axis=-1, keepdims=True))
    ds_bf16 = (d_s * SCALE).astype(jnp.bfloat16).astype(jnp.float32)
    d_q = jnp.einsum("bkgst,btke->bskge", ds_bf16, k_grid).astype(jnp.bfloat16).reshape(ROWS, Q_WIDTH)
    d_k = jnp.einsum("bkgst,bskge->btke", ds_bf16, q_grid).astype(jnp.bfloat16).reshape(ROWS, KV_WIDTH)
    d_v = d_v.reshape(ROWS, KV_WIDTH)
    d_q_w = matmul(normed.T, d_q)
    d_k_w = matmul(normed.T, d_k)
    d_v_w = matmul(normed.T, d_v)
    d_norm = matmul(d_q, q_mat.T) + matmul(d_k, k_mat.T) + matmul(d_v, v_mat.T)
    grad_x = (grad_y.astype(jnp.float32) + norm_back(x_blk, d_norm)).astype(jnp.bfloat16)
    return (grad_x, d_q_w.reshape(D, HEADS, HEAD), d_k_w.reshape(D, KV_HEADS, HEAD),
            d_v_w.reshape(D, KV_HEADS, HEAD), d_o_w.reshape(D, HEADS, HEAD))


def mlp_forward(x_blk, up_weight, down_weight):
    normed = norm_bf16(x_blk)
    gelu_act = jax.nn.gelu(matmul(normed, up_weight)).astype(jnp.bfloat16)
    return (x_blk.astype(jnp.float32) + matmul(gelu_act, down_weight)).astype(jnp.bfloat16)


def mlp_backward(x_blk, up_weight, down_weight, grad_y):
    normed = norm_bf16(x_blk)
    gelu_f32, gelu_pull = jax.vjp(jax.nn.gelu, matmul(normed, up_weight))
    gelu_act = gelu_f32.astype(jnp.bfloat16)
    d_down = matmul(gelu_act.T, grad_y)
    d_hid = gelu_pull(matmul(grad_y, down_weight.T))[0].astype(jnp.bfloat16)
    d_up = matmul(normed.T, d_hid)
    d_norm = matmul(d_hid, up_weight.T)
    grad_x = (grad_y.astype(jnp.float32) + norm_back(x_blk, d_norm)).astype(jnp.bfloat16)
    return grad_x, d_up, d_down


def block_pass(x_blk, g_blk, weights):
    def fwd_step(carry_x, layer_w):
        q_weight, k_weight, v_weight, o_weight, up_weight, down_weight = layer_w
        mid_act = attn_forward(carry_x, q_weight, k_weight, v_weight, o_weight)
        out_act = mlp_forward(mid_act, up_weight, down_weight)
        return out_act, (carry_x, mid_act)

    y_blk, (attn_in, mlp_in) = lax.scan(fwd_step, x_blk, weights)

    def bwd_step(grad_act, packed):
        q_weight, k_weight, v_weight, o_weight, up_weight, down_weight, attn_x, mlp_x = packed
        grad_mid, d_up, d_down = mlp_backward(mlp_x, up_weight, down_weight, grad_act)
        grad_in, d_q, d_k, d_v, d_o = attn_backward(attn_x, q_weight, k_weight, v_weight, o_weight, grad_mid)
        return grad_in, (d_q, d_k, d_v, d_o, d_up, d_down)

    dx_blk, grads = lax.scan(bwd_step, g_blk, weights + (attn_in, mlp_in), reverse=True)
    return y_blk, dx_blk, grads


def reference(x_in, w_q, w_k, w_v, w_o, w_up, w_down, grad_out):
    weights = (w_q, w_k, w_v, w_o, w_up, w_down)
    x_blocks = x_in.reshape(BLOCKS, ROWS, D)
    g_blocks = grad_out.reshape(BLOCKS, ROWS, D)
    zero_grads = tuple(jnp.zeros(weight.shape, jnp.float32) for weight in weights)

    def block_step(acc_grads, pair_blk):
        y_blk, dx_blk, grads = block_pass(pair_blk[0], pair_blk[1], weights)
        acc_grads = tuple(prev_sum + block_grad for prev_sum, block_grad in zip(acc_grads, grads))
        return acc_grads, (y_blk, dx_blk)

    totals, (y_all, dx_all) = lax.scan(block_step, zero_grads, (x_blocks, g_blocks))
    return (y_all.reshape(SEQS, SEQ, D), dx_all.reshape(SEQS, SEQ, D),
            totals[0], totals[1], totals[2], totals[3], totals[4], totals[5])
```

```python
import functools

import jax
import jax.numpy as jnp
from jax import lax
from jax.experimental import pallas as pl
from jax.experimental.pallas import tpu as pltpu
from jax.sharding import PartitionSpec as P

AXES = ("sub", "fsdp")
MESH = pl.DeviceIdType.MESH
EPS = 1e-6
MASK_FILL = -1e30
F32 = jnp.float32
BF16 = jnp.bfloat16
SIDE = 4


class Comm:
    def __init__(self, send_sem, recv_sem, copy_sem):
        self.send_sem, self.recv_sem, self.copy_sem = send_sem, recv_sem, copy_sem
        self.sent, self.copies = [], 0
        fsdp = lax.axis_index("fsdp")
        self.pos = {
            "x": lax.axis_index("sub"),
            "z": fsdp // (2 * SIDE),
            "y": lax.rem(fsdp // 2, SIDE),
            "c": lax.rem(fsdp, 2),
        }

    def at(self, axis, shift):
        if axis == "c":
            return 1 - self.pos["c"]
        return lax.rem(self.pos[axis] + (shift + SIDE), SIDE)

    def device(self, axis, shift):
        place = dict(self.pos)
        place[axis] = self.at(axis, shift)
        return {"sub": place["x"], "fsdp": (place["z"] * SIDE + place["y"]) * 2 + place["c"]}

    def remote(self, source, target, axis, shift=0):
        index = len(self.sent)
        copy = pltpu.make_async_remote_copy(
            src_ref=source, dst_ref=target, send_sem=self.send_sem.at[index], recv_sem=self.recv_sem.at[index],
            device_id=self.device(axis, shift), device_id_type=MESH)
        copy.start()
        self.sent.append(copy)
        return copy

    def local(self, source, target):
        copy = pltpu.make_async_copy(source, target, self.copy_sem.at[self.copies])
        copy.start()
        self.copies += 1
        return copy

    def finish(self):
        for copy in self.sent:
            copy.wait_send()


def add_into(target, source):
    shape = target.shape
    rows = shape[-2]
    step = 8
    lead = shape[:-2]
    total = 1
    for size in lead:
        total *= size

    def body(index, carry):
        row = pl.multiple_of(lax.rem(index, rows // step) * step, step)
        rest = index // (rows // step)
        where = []
        for size in reversed(lead):
            where.append(lax.rem(rest, size))
            rest = rest // size
        where = tuple(where[::-1]) + (pl.ds(row, step), slice(None))
        target[where] = target[where] + source[where]
        return carry

    lax.fori_loop(0, total * (rows // step), body, 0)


def lead_half(view, part):
    size = view.shape[0] // 2
    return view.at[pl.ds(part * size, size)]


def lane_half(view, part):
    size = view.shape[-1] // 2
    return view.at[(slice(None),) * (len(view.shape) - 1) + (pl.ds(part * size, size),)]


def half_shape(shape, half):
    if half is lead_half:
        return (shape[0] // 2,) + tuple(shape[1:])
    return tuple(shape[:-1]) + (shape[-1] // 2,)


def ring_gather(comm, axis, block, half, own=None):
    here, left, right, far = comm.at(axis, 0), comm.at(axis, -1), comm.at(axis, 1), comm.at(axis, 2)
    source = block(here) if own is None else own
    from_left = comm.remote(source, block(here), axis, 1)
    from_right = comm.remote(source, block(here), axis, -1)
    yield
    from_left.wait_recv()
    far_low = comm.remote(half(block(left), 0), half(block(left), 0), axis, 1)
    yield
    from_right.wait_recv()
    far_high = comm.remote(half(block(right), 1), half(block(right), 1), axis, -1)
    yield
    far_low.wait_recv()
    far_high.wait_recv()


def ring_scatter_shapes(shape, half, staged):
    small = half_shape(shape, half)
    buffers = [small, small, shape, shape]
    if staged:
        buffers += [small, small, shape]
    return [pltpu.VMEM(size, F32) for size in buffers]


def ring_scatter(comm, axis, part, half, buffers, staged):
    low_in, high_in, left_in, right_in = buffers[:4]
    here, left, right, far = (part(comm.at(axis, shift)) for shift in (0, -1, 1, 2))
    low = comm.remote(half(far, 0), low_in, axis, 1)
    high = comm.remote(half(far, 1), high_in, axis, -1)
    right_high = comm.remote(half(right, 1), half(left_in, 1), axis, 1)
    left_low = comm.remote(half(left, 0), half(right_in, 0), axis, -1)
    if staged:
        low_own, high_own, total = buffers[4:]
        loads = [comm.local(half(right, 0), low_own), comm.local(half(left, 1), high_own), comm.local(here, total)]
    else:
        low_own, high_own, total = half(right, 0), half(left, 1), here
        loads = [None, None, None]
    yield
    if staged:
        loads[0].wait()
    low.wait_recv()
    add_into(low_own, low_in)
    right_low = comm.remote(low_own, half(left_in, 0), axis, 1)
    yield
    if staged:
        loads[1].wait()
    high.wait_recv()
    add_into(high_own, high_in)
    left_high = comm.remote(high_own, half(right_in, 1), axis, -1)
    yield
    if staged:
        loads[2].wait()
    right_high.wait_recv()
    right_low.wait_recv()
    add_into(total, left_in)
    yield
    left_low.wait_recv()
    left_high.wait_recv()
    add_into(total, right_in)
    return total


class GatherTokens:
    neighbours = (("c", 0), ("x", 1), ("x", -1))
    remotes, locals = 9, 1

    def __init__(self, tokens):
        self.operands = (tokens,)
        self.in_specs = [pl.BlockSpec(memory_space=pltpu.VMEM)]
        self.out_shapes = [jax.ShapeDtypeStruct((SIDE, 2) + tokens.shape, tokens.dtype)]
        self.out_specs = [pl.BlockSpec(memory_space=pl.ANY)]
        self.scratch = []

    def body(self, comm, ins, outs, scratch):
        own, full = ins[0], outs[0]
        core = comm.pos["c"]
        here, left, right, far = (comm.at("x", shift) for shift in (0, -1, 1, 2))
        stored = comm.local(own, full.at[here, core])
        from_left = comm.remote(own, full.at[here, core], "x", 1)
        from_right = comm.remote(own, full.at[here, core], "x", -1)
        waits = [comm.remote(own, full.at[here, core], "c")]
        yield
        from_left.wait_recv()
        far_low = comm.remote(lead_half(full.at[left, core], 0), lead_half(full.at[left, core], 0), "x", 1)
        waits.append(comm.remote(full.at[left, core], full.at[left, core], "c"))
        yield
        from_right.wait_recv()
        far_high = comm.remote(lead_half(full.at[right, core], 1), lead_half(full.at[right, core], 1), "x", -1)
        waits.append(comm.remote(full.at[right, core], full.at[right, core], "c"))
        yield
        for index, copy in enumerate((far_low, far_high)):
            copy.wait_recv()
            view = lead_half(full.at[far, core], index)
            waits.append(comm.remote(view, view, "c"))
        yield
        stored.wait()
        for copy in waits:
            copy.wait_recv()


class ScatterTokens:
    neighbours = (("c", 0), ("x", 1), ("x", -1))
    remotes, locals = 10, 4

    def __init__(self, terms):
        rows, width = terms.shape[2:]
        self.operands = (terms,)
        self.in_specs = [pl.BlockSpec(memory_space=pl.ANY)]
        self.out_shapes = [jax.ShapeDtypeStruct((rows, width), F32)]
        self.out_specs = [pl.BlockSpec(memory_space=pltpu.VMEM)]
        self.scratch = [pltpu.VMEM((SIDE, rows, width), F32), pltpu.VMEM((SIDE, rows, width), F32)]
        self.scratch += ring_scatter_shapes((rows, width), lead_half, False)

    def body(self, comm, ins, outs, scratch):
        terms, total = ins[0], outs[0]
        own, other, low_in, high_in, left_in, right_in = scratch
        core = comm.pos["c"]
        loads, arrivals = {}, {}
        for shift in (2, 1, 3, 0):
            target = comm.at("x", shift)
            arrivals[shift] = comm.remote(terms.at[target, 1 - core], other.at[shift], "c")
            loads[shift] = comm.local(terms.at[target, core], own.at[shift])

        def pair(shift):
            loads[shift].wait()
            arrivals[shift].wait_recv()
            add_into(own.at[shift], other.at[shift])

        yield
        pair(2)
        low = comm.remote(lead_half(own.at[2], 0), low_in, "x", 1)
        high = comm.remote(lead_half(own.at[2], 1), high_in, "x", -1)
        yield
        pair(1)
        right_high = comm.remote(lead_half(own.at[1], 1), lead_half(left_in, 1), "x", 1)
        yield
        pair(3)
        left_low = comm.remote(lead_half(own.at[3], 0), lead_half(right_in, 0), "x", -1)
        yield
        low.wait_recv()
        add_into(lead_half(own.at[1], 0), low_in)
        right_low = comm.remote(lead_half(own.at[1], 0), lead_half(left_in, 0), "x", 1)
        yield
        high.wait_recv()
        add_into(lead_half(own.at[3], 1), high_in)
        left_high = comm.remote(lead_half(own.at[3], 1), lead_half(right_in, 1), "x", -1)
        yield
        pair(0)
        yield
        right_high.wait_recv()
        right_low.wait_recv()
        add_into(own.at[0], left_in)
        yield
        left_low.wait_recv()
        left_high.wait_recv()
        add_into(own.at[0], right_in)
        rows = total.shape[0]

        def store(index, carry):
            where = pl.ds(pl.multiple_of(index * 8, 8), 8)
            total[where, :] = own[0, where, :]
            return carry

        lax.fori_loop(0, rows // 8, store, 0)


class GatherPlane:
    def __init__(self, shard, order, along_x=False, half=lead_half):
        self.order, self.along_x, self.half = order, along_x, half
        self.neighbours = tuple((axis, shift) for axis in "zy" for shift in (1, -1))
        if along_x:
            self.neighbours += (("x", 1), ("x", -1))
        self.remotes, self.locals = (12 if along_x else 8), 1
        self.operands = (shard,)
        self.in_specs = [pl.BlockSpec(memory_space=pltpu.VMEM)]
        lead = SIDE if along_x else shard.shape[0]
        self.out_shapes = [jax.ShapeDtypeStruct((lead, SIDE, SIDE) + shard.shape[-2:], shard.dtype)]
        self.out_specs = [pl.BlockSpec(memory_space=pl.ANY)]
        self.scratch = []

    def body(self, comm, ins, outs, scratch):
        shard, full = ins[0], outs[0]
        z, y = comm.pos["z"], comm.pos["y"]
        if self.along_x:
            stored = comm.local(shard, full.at[comm.pos["x"], z, y])
            yield from ring_gather(comm, "x", lambda i: full.at[i, z, y], lane_half, shard)
            stored.wait()
        else:
            comm.local(shard, full.at[:, z, y]).wait()
        first, second = self.order
        if first == "y":
            yield from ring_gather(comm, "y", lambda i: full.at[:, z, i], self.half)
            yield from ring_gather(comm, "z", lambda i: full.at[:, i], self.half)
        else:
            yield from ring_gather(comm, "z", lambda i: full.at[:, i, y], self.half)
            yield from ring_gather(comm, "y", lambda i: full.at[:, :, i], self.half)


class ScatterPlane:
    def __init__(self, terms, order, along_x=False, half=lead_half):
        self.order, self.along_x, self.half = order, along_x, half
        self.neighbours = tuple((axis, shift) for axis in "zy" for shift in (1, -1))
        if along_x:
            self.neighbours += (("x", 1), ("x", -1))
        self.remotes, self.locals = (18 if along_x else 12), 4
        lead, _, _, rows, width = terms.shape
        self.operands = (terms,)
        self.in_specs = [pl.BlockSpec(memory_space=pl.ANY)]
        shape = (rows, width) if along_x else (lead, rows, width)
        self.out_shapes = [jax.ShapeDtypeStruct(shape, F32)]
        self.out_specs = [pl.BlockSpec(memory_space=pl.ANY)]
        self.scratch = ring_scatter_shapes((lead, SIDE, rows, width), half, True)
        self.scratch += ring_scatter_shapes((lead, rows, width), half, False)
        if along_x:
            self.scratch += ring_scatter_shapes((rows, width), lane_half, False)

    def body(self, comm, ins, outs, scratch):
        terms, result = ins[0], outs[0]
        first, second = self.order
        if first == "y":
            part = lambda i: terms.at[:, :, i]
        else:
            part = lambda i: terms.at[:, i]
        total = yield from ring_scatter(comm, first, part, self.half, scratch[:7], True)
        total = yield from ring_scatter(comm, second, lambda i: total_at(total, i), self.half, scratch[7:11], False)
        if self.along_x:
            last = total
            total = yield from ring_scatter(comm, "x", lambda i: last.at[i], lane_half, scratch[11:15], False)
        comm.local(total, result).wait()


def total_at(total, index):
    return total.at[:, index]


def communicate(name, collective_id, *streams):
    neighbours = []
    for stream in streams:
        neighbours += [place for place in stream.neighbours if place not in neighbours]
    remotes = sum(stream.remotes for stream in streams)
    copies = sum(stream.locals for stream in streams)
    counts = [(len(stream.operands), len(stream.out_shapes), len(stream.scratch)) for stream in streams]

    def kernel(*refs):
        refs = list(refs)
        take = lambda count: [refs.pop(0) for _ in range(count)]
        ins = [take(count[0]) for count in counts]
        outs = [take(count[1]) for count in counts]
        scratch = [take(count[2]) for count in counts]
        comm = Comm(*refs)
        barrier = pltpu.get_barrier_semaphore()
        for axis, shift in neighbours:
            pl.semaphore_signal(barrier, inc=1, device_id=comm.device(axis, shift), device_id_type=MESH)
        pl.semaphore_wait(barrier, len(neighbours))
        running = [stream.body(comm, *where) for stream, where in zip(streams, zip(ins, outs, scratch))]
        while running:
            for stream in list(running):
                try:
                    next(stream)
                except StopIteration:
                    running.remove(stream)
        comm.finish()

    results = pl.pallas_call(
        kernel,
        out_shape=[shape for stream in streams for shape in stream.out_shapes],
        in_specs=[spec for stream in streams for spec in stream.in_specs],
        out_specs=[spec for stream in streams for spec in stream.out_specs],
        scratch_shapes=[shape for stream in streams for shape in stream.scratch]
        + [pltpu.SemaphoreType.DMA((remotes,)), pltpu.SemaphoreType.DMA((remotes,)), pltpu.SemaphoreType.DMA((copies,))],
        compiler_params=pltpu.CompilerParams(
            collective_id=collective_id, has_side_effects=True, vmem_limit_bytes=60 * 1024 * 1024),
        name=name,
    )(*[operand for stream in streams for operand in stream.operands])
    return list(results)


def rms_norm(values):
    return values * lax.rsqrt(jnp.mean(values * values, axis=-1, keepdims=True) + EPS)


def norm_bf16(x_loc):
    return rms_norm(x_loc.astype(F32)).astype(BF16)


def norm_back(x_loc, grad_norm):
    _, pull_back = jax.vjp(rms_norm, x_loc.astype(F32))
    return pull_back(grad_norm)[0]


def mixed(form, left, right):
    return jnp.einsum(form, left, right, preferred_element_type=F32)


def swap_pairs(mesh):
    return [(index, index ^ 1) for index in range(mesh.shape["fsdp"])]


def solution(mesh):
    swap = swap_pairs(mesh)

    def trade(values):
        return lax.ppermute(values, "fsdp", swap)

    def pick(values, index):
        return lax.dynamic_index_in_dim(values, index, 0, keepdims=False)

    def both(own, other, core):
        return jnp.where(core == 0, jnp.stack([own, other]), jnp.stack([other, own]))

    def body(x_loc, w_q, w_k, w_v, w_o, w_up, w_down, grad_out):
        core = lax.rem(lax.axis_index("fsdp"), 2)
        pairs, part_rows, heads, head = w_q.shape
        width = part_rows * mesh.shape["sub"] * mesh.shape["fsdp"]
        kv_heads = w_k.shape[2]
        group = heads // kv_heads
        q_cols = group * head
        seq = x_loc.shape[1]
        scale = head ** -0.5
        ff_part = w_down.shape[1]
        ff_pad = -(-ff_part // 8) * 8
        planes = SIDE * SIDE
        ff_core = planes * ff_pad

        w_attn = jnp.concatenate([
            w_q.reshape(pairs, part_rows, kv_heads, q_cols), w_k, w_v,
            w_o.reshape(pairs, part_rows, kv_heads, q_cols)], axis=3).transpose(2, 0, 1, 3)
        given = pick(w_attn, 1 - core)
        kept = pick(w_attn, core)
        taken = trade(given)
        attn_shard = both(kept, taken, core).transpose(1, 0, 2, 3).reshape(pairs, 2 * part_rows, 2 * q_cols + 2 * head)
        qkv_cols = q_cols + 2 * head
        qkv_shard, o_shard = attn_shard[:, :, :qkv_cols], attn_shard[:, :, qkv_cols:]

        up = w_up.reshape(pairs, part_rows, SIDE, planes, 2, ff_part)
        up = jnp.pad(up, ((0, 0),) * 5 + ((0, ff_pad - ff_part),))
        up = up.transpose(2, 4, 0, 1, 3, 5).reshape(SIDE, 2, pairs, part_rows, ff_core)
        up = lax.all_to_all(up, "sub", 0, 0, tiled=True).transpose(1, 0, 2, 3, 4)
        taken = trade(pick(up, 1 - core))
        up_shard = both(pick(up, core), taken, core)
        up_shard = up_shard.transpose(2, 1, 0, 3, 4).reshape(pairs, SIDE, 2 * part_rows, ff_core)
        down_shard = jnp.pad(w_down, ((0, 0), (0, ff_pad - ff_part), (0, 0)))[:, None]

        def gather_attn(layer):
            return (GatherPlane(qkv_shard[layer], "yz", along_x=True), GatherPlane(o_shard[layer], "zy", along_x=True))

        def gather_mlp(layer):
            return (GatherPlane(up_shard[layer], "zy"), GatherPlane(down_shard[layer], "yz", half=lane_half))

        def attn_weights(parts):
            return parts[0].reshape(width, qkv_cols), parts[1].reshape(width, q_cols)

        def mlp_weights(parts):
            return parts[0].reshape(width, ff_core), parts[1].reshape(ff_core, width)

        positions = jnp.arange(seq)
        causal = positions[:, None] >= positions[None, :]

        def attn_forward(x_own, qkv_w, o_w):
            normed = norm_bf16(x_own[0])
            normed = both(normed, trade(normed), core)
            qkv = mixed("bsd,dh->bsh", normed, qkv_w).astype(BF16)
            q_act = qkv[:, :, :q_cols].reshape(2, seq, group, head)
            k_act, v_act = qkv[:, :, q_cols:q_cols + head], qkv[:, :, q_cols + head:]
            scores = mixed("bsge,bte->bgst", q_act, k_act) * scale
            p_float = jax.nn.softmax(jnp.where(causal, scores, MASK_FILL), axis=-1)
            p_bf16 = p_float.astype(BF16)
            o_act = mixed("bgst,bte->bsge", p_bf16, v_act).astype(BF16).reshape(2, seq, q_cols)
            terms = mixed("bsh,dh->bsd", o_act, o_w)
            proj = pick(terms, core) + trade(pick(terms, 1 - core))
            return (x_own.astype(F32) + proj).astype(BF16), (x_own, normed, q_act, k_act, v_act, p_float, p_bf16, o_act)

        def attn_backward(saved, qkv_w, o_w, grad_y):
            x_own, normed, q_act, k_act, v_act, p_float, p_bf16, o_act = saved
            grads = both(grad_y[0], trade(grad_y[0]), core)
            d_o_w = mixed("bsd,bsh->dh", grads, o_act)
            d_o = mixed("bsd,dh->bsh", grads, o_w).astype(BF16).reshape(2, seq, group, head)
            d_p = mixed("bsge,bte->bgst", d_o, v_act)
            d_v = mixed("bgst,bsge->bte", p_bf16, d_o).astype(BF16)
            d_s = p_float * (d_p - jnp.sum(p_float * d_p, axis=-1, keepdims=True))
            ds_bf16 = (d_s * scale).astype(BF16)
            d_q = mixed("bgst,bte->bsge", ds_bf16, k_act).astype(BF16).reshape(2, seq, q_cols)
            d_k = mixed("bgst,bsge->bte", ds_bf16, q_act).astype(BF16)
            d_qkv = jnp.concatenate([d_q, d_k, d_v], axis=2)
            d_qkv_w = mixed("bsd,bsh->dh", normed, d_qkv)
            terms = mixed("bsh,dh->bsd", d_qkv, qkv_w)
            d_norm = pick(terms, core) + trade(pick(terms, 1 - core))
            grad_x = (grad_y.astype(F32) + norm_back(x_own, d_norm[None])).astype(BF16)
            return grad_x, d_qkv_w, d_o_w

        tokens = SIDE * 2 * seq

        def scatter_attn(d_qkv_w, d_o_w):
            shape = (SIDE, SIDE, SIDE, 2 * part_rows)
            return (ScatterPlane(d_qkv_w.reshape(shape + (qkv_cols,)), "yz", along_x=True),
                    ScatterPlane(d_o_w.reshape(shape + (q_cols,)), "zy", along_x=True))

        def scatter_mlp(d_up_w, d_down_w):
            return (ScatterPlane(d_up_w.reshape(SIDE, SIDE, SIDE, 2 * part_rows, ff_core), "zy"),
                    ScatterPlane(d_down_w.reshape(1, SIDE, SIDE, ff_pad, width), "yz", half=lane_half))

        attn_w, mlp_w, attn_saved, mlp_saved = [], [], [], []
        carry_x = x_loc
        attn_w.append(attn_weights(communicate("gather_attn", 0, *gather_attn(0))))
        for layer in range(pairs):
            carry_x, saved = attn_forward(carry_x, *attn_w[layer])
            attn_saved.append(saved)
            normed = norm_bf16(carry_x[0])
            parts = communicate("gather_tokens_mlp", 1, GatherTokens(normed), *gather_mlp(layer))
            normed = parts[0].reshape(tokens, width)
            up_w, down_w = mlp_weights(parts[1:])
            mlp_w.append((up_w, down_w))
            hidden = mixed("td,df->tf", normed, up_w)
            gelu_act = jax.nn.gelu(hidden).astype(BF16)
            terms = mixed("tf,fd->td", gelu_act, down_w).reshape(SIDE, 2, seq, width)
            mlp_saved.append((carry_x, normed, hidden))
            if layer + 1 < pairs:
                parts = communicate("scatter_tokens_attn", 2, ScatterTokens(terms), *gather_attn(layer + 1))
                attn_w.append(attn_weights(parts[1:]))
            else:
                parts = communicate("scatter_tokens", 3, ScatterTokens(terms))
            carry_x = (carry_x.astype(F32) + parts[0][None]).astype(BF16)
        y_loc = carry_x

        grad_x = grad_out
        attn_sums, mlp_sums = [None] * pairs, [None] * pairs
        waiting = None
        for layer in reversed(range(pairs)):
            x_own, normed, hidden = mlp_saved[layer]
            up_w, down_w = mlp_w[layer]
            if waiting is None:
                parts = communicate("gather_tokens", 4, GatherTokens(grad_x[0]))
            else:
                parts = communicate("gather_tokens_sum", 5, GatherTokens(grad_x[0]), waiting[1])
                sum_o = parts[1]
            grads = parts[0].reshape(tokens, width)
            gelu_f32, gelu_pull = jax.vjp(jax.nn.gelu, hidden)
            gelu_act = gelu_f32.astype(BF16)
            d_hid = gelu_pull(mixed("td,fd->tf", grads, down_w))[0].astype(BF16)
            terms = mixed("tf,df->td", d_hid, up_w).reshape(SIDE, 2, seq, width)
            d_down_w = mixed("tf,td->fd", gelu_act, grads)
            d_up_w = mixed("td,tf->df", normed, d_hid)
            if waiting is None:
                parts = communicate("scatter_tokens_mlp", 6, ScatterTokens(terms), *scatter_mlp(d_up_w, d_down_w))
                mlp_sums[layer] = parts[1:]
            else:
                parts = communicate("scatter_tokens_sum", 7, ScatterTokens(terms), waiting[0])
                attn_sums[layer + 1] = (parts[1], sum_o)
            grad_x = (grad_x.astype(F32) + norm_back(x_own, parts[0][None])).astype(BF16)
            grad_x, d_qkv_w, d_o_w = attn_backward(attn_saved[layer], *attn_w[layer], grad_x)
            waiting = scatter_attn(d_qkv_w, d_o_w)
        parts = communicate("scatter_last", 8, *scatter_mlp(d_up_w, d_down_w), *waiting)
        mlp_sums[0], attn_sums[0] = parts[:2], parts[2:]

        attn_sum = jnp.concatenate([jnp.stack([sums[0] for sums in attn_sums]), jnp.stack([sums[1] for sums in attn_sums])],
                                   axis=2).reshape(pairs, 2, part_rows, qkv_cols + q_cols).transpose(1, 0, 2, 3)
        taken = trade(pick(attn_sum, 1 - core))
        attn_sum = both(pick(attn_sum, core), taken, core).transpose(1, 2, 0, 3)
        d_q = attn_sum[..., :q_cols].reshape(w_q.shape)
        d_k = attn_sum[..., q_cols:q_cols + head]
        d_v = attn_sum[..., q_cols + head:qkv_cols]
        d_o = attn_sum[..., qkv_cols:].reshape(w_o.shape)
        d_down = jnp.stack([sums[1][0, :ff_part] for sums in mlp_sums])
        d_up = jnp.stack([sums[0] for sums in mlp_sums]).reshape(pairs, SIDE, 2, part_rows, ff_core)
        d_up = d_up.transpose(2, 1, 0, 3, 4)
        taken = trade(pick(d_up, 1 - core))
        d_up = both(pick(d_up, core), taken, core).transpose(1, 0, 2, 3, 4)
        d_up = lax.all_to_all(d_up, "sub", 0, 0, tiled=True)
        d_up = d_up.reshape(SIDE, 2, pairs, part_rows, planes, ff_pad)[..., :ff_part]
        d_up = d_up.transpose(2, 3, 0, 4, 1, 5).reshape(w_up.shape)
        return y_loc, grad_x, d_q, d_k, d_v, d_o, d_up, d_down

    row_spec = P(AXES)
    weight_spec = P(None, AXES)
    return jax.shard_map(body, mesh=mesh, in_specs=(row_spec,) + (weight_spec,) * 6 + (row_spec,),
                         out_specs=(row_spec, row_spec) + (weight_spec,) * 6, check_vma=False)
```
